32 devices in a mesh: orient: 4 (over z), slab: 8 (over y, x, core).
Axes of the slice: x: 2, y: 2, z: 4, core: 2. Of those that a mesh axis runs over, the one named last changes fastest.
Arguments:
- polarization: bfloat16 [8, 2, 3, 8, 9216], P('orient', None, None, 'slab'), may hold values from -6 to 6
- occupied: int32 [8, 9216], P('slab'), may hold values from 0 to 1, as said below
- orient_table: int32 [8, 2], replicated, may hold values from 0 to 15
- dir_index: int32 [2048, 2], replicated, may hold values from 0 to 179
Outputs:
- mueller: float32 [4, 2048], P(None, 'slab')
The draws below stay inside these ranges and needn't reach their ends.
Inputs may be any that keep to these rules, and one draw needn't show every extreme that they name: 1 marks an occupied dipole cell.
All inputs are finite; a program needn't handle non-finite values.
Results may differ from the reference program's by a relative error of at most 0.00087.
Values may be sent and summed in bfloat16 or wider, within the bound.
A program may use at most 64 MiB of HBM per device.

```python
import math
import jax
import jax.numpy as jnp
from jax import lax

GX = 96
GY = 96
DIRS = 2048
ORIENT_GRID = 16
THETA_GRID = 180
GXY = 9216
GZ = 8
ORIENTS = 8


def draw_occupied(key, part):
    first_key = jax.random.fold_in(key, 11)
    second_key = jax.random.fold_in(key, 23)
    radius = jax.random.randint(first_key, (), 3 * GX // 4, GX + 1)
    planes_iota = jnp.arange(GZ, dtype=jnp.int32)[:, None]
    cells_iota = jnp.arange(GX * GY, dtype=jnp.int32)[None, :]
    offset_x = 2 * (cells_iota % GX) + 1 - GX
    offset_y = 2 * (cells_iota // GX) + 1 - GY
    offset_z = (2 * planes_iota + 1 - GZ) * GX // GZ
    inside = offset_x * offset_x + offset_y * offset_y + offset_z * offset_z <= radius * radius
    keeper = jax.random.randint(second_key, (GZ, GX * GY), 0, 8) != 0
    return (inside & keeper).astype(jnp.int32)


def with_ends(array, own_key, least, high):
    longest = array.shape.index(max(array.shape))
    spots = []
    for shift in (0, 1):
        where = [jax.random.randint(jax.random.fold_in(own_key, axis), (), 0, length) for axis, length in enumerate(array.shape)]
        where[longest] = (where[longest] + shift) % array.shape[longest]
        spots.append(tuple(where))
    return array.at[spots[0]].set(least).at[spots[1]].set(high)


def steps_of(rng, dims, pieces, least, top_value):
    def one(axis_at, blocks):
        steps = jax.random.uniform(jax.random.fold_in(jax.random.fold_in(rng, 6), axis_at), (blocks,), jnp.float32, least / len(pieces), top_value / len(pieces))
        return jnp.repeat(jnp.exp(steps), dims[axis_at] // blocks).reshape((-1,) + (1,) * (len(dims) - axis_at - 1))

    level = one(*pieces[0])
    for cut in pieces[1:]:
        level = level * one(*cut)
    return level


def normal_values(rng, extent, scale, limit, cuts=(), held_as=jnp.bfloat16):
    factor_of = steps_of(rng, extent, cuts, -0.22, 0.18) if cuts else 1.0
    values = jax.random.normal(rng, extent, jnp.float32) * scale * factor_of
    return jnp.minimum(jnp.maximum(values, -limit), limit).astype(held_as)


def setup_inputs(seed: int = 0) -> dict:
    streams_of = jax.random.split(jax.random.key(seed), 5)
    polarization = normal_values(streams_of[0], (ORIENTS, 2, 3, GZ, GXY), 1.0, 6.0, ((0, 4), (3, 8)))
    occupied = draw_occupied(jax.random.fold_in(streams_of[4], 71), 0)
    orient_table = with_ends(jax.random.randint(streams_of[2], (ORIENTS, 2), 0, ORIENT_GRID), jax.random.fold_in(streams_of[2], 1), 0, ORIENT_GRID - 1).astype(jnp.int32)
    dir_index = with_ends(jax.random.randint(streams_of[3], (DIRS, 2), 0, THETA_GRID), jax.random.fold_in(streams_of[3], 1), 0, THETA_GRID - 1).astype(jnp.int32)
    return {"polarization": polarization, "occupied": occupied, "orient_table": orient_table, "dir_index": dir_index}


wave_step = 0.4


def direction_angles(dir_index):
    polar_angle = (dir_index[:, 0].astype(jnp.float32) + 0.5) * (math.pi / THETA_GRID)
    azimuth = dir_index[:, 1].astype(jnp.float32) * (2.0 * math.pi / THETA_GRID)
    return polar_angle, azimuth


def unit_vectors(polar_angle, azimuth):
    return (jnp.sin(polar_angle) * jnp.cos(azimuth), jnp.sin(polar_angle) * jnp.sin(azimuth), jnp.cos(polar_angle))


def phase_block(within, plane_index, normals):
    xcoord = (within % GX).astype(jnp.float32)
    ycoord = (within // GX).astype(jnp.float32)
    zcoord = plane_index.astype(jnp.float32)
    angle = wave_step * (xcoord[:, None] * normals[0][None, :] + ycoord[:, None] * normals[1][None, :] + zcoord[:, None] * normals[2][None, :])
    return jnp.concatenate([jnp.cos(angle), -jnp.sin(angle)], axis=1).astype(jnp.bfloat16)


def orient_weights(orient_table):
    turn_angle = orient_table[:, 0].astype(jnp.float32) * (2.0 * math.pi / ORIENT_GRID)
    weight = jnp.sin((orient_table[:, 1].astype(jnp.float32) + 0.5) * (math.pi / ORIENT_GRID))
    return turn_angle, weight


def mueller_sum(amplitude, orient_table, polar_angle, azimuth):
    turn_angle, weight = orient_weights(orient_table)
    relative = azimuth[None, :] - turn_angle[:, None]
    cos_polar = jnp.cos(polar_angle)[None, :]
    sin_polar = jnp.sin(polar_angle)[None, :]
    cos_turn = jnp.cos(relative)
    sin_turn = jnp.sin(relative)
    parallel = (cos_polar * cos_turn, cos_polar * sin_turn, -sin_polar)
    across = (-sin_turn, cos_turn, None)

    def project(polar_index, basis_set):
        summed = amplitude[:, polar_index, 0] * basis_set[0][:, None, :] + amplitude[:, polar_index, 1] * basis_set[1][:, None, :]
        if basis_set[2] is not None:
            summed = summed + amplitude[:, polar_index, 2] * basis_set[2][:, None, :]
        return summed

    def square(values):
        return values[:, 0] * values[:, 0] + values[:, 1] * values[:, 1]

    lower_right = project(1, across)
    upper_left = project(0, parallel)
    upper_right = project(0, across)
    lower_left = project(1, parallel)
    elem_total = 0.5 * (square(lower_right) + square(upper_left) + square(upper_right) + square(lower_left))
    elem_diff = 0.5 * (square(upper_left) - square(lower_right) + square(lower_left) - square(upper_right))
    elem_real = (lower_right[:, 0] * upper_left[:, 0] + lower_right[:, 1] * upper_left[:, 1]
                 + upper_right[:, 0] * lower_left[:, 0] + upper_right[:, 1] * lower_left[:, 1])
    elem_imag = (upper_left[:, 1] * lower_right[:, 0] - upper_left[:, 0] * lower_right[:, 1]
                 + lower_left[:, 1] * upper_right[:, 0] - lower_left[:, 0] * upper_right[:, 1])
    stacked = jnp.stack([elem_total, elem_diff, elem_real, elem_imag])
    return jnp.sum(stacked * weight[None, :, None], axis=1)


def reference(polarization, occupied, orient_table, dir_index):
    polar_angle, azimuth = direction_angles(dir_index)
    normals = unit_vectors(polar_angle, azimuth)
    masked = polarization * occupied.astype(jnp.bfloat16)[None, None, None]
    cells_all = GZ * GXY
    flattened = masked.reshape(ORIENTS * 6, cells_all)
    block_size = math.gcd(cells_all, 4096)

    def accumulate(summed, block_index):
        offset = block_index * block_size
        segment = lax.dynamic_slice_in_dim(flattened, offset, block_size, 1)
        cell_index = offset + jnp.arange(block_size, dtype=jnp.int32)
        phase = phase_block(cell_index % GXY, cell_index // GXY, normals)
        return summed + jnp.dot(segment, phase, preferred_element_type=jnp.float32), None

    initial = jnp.zeros((ORIENTS * 6, 2 * DIRS), jnp.float32)
    amplitude = lax.scan(accumulate, initial, jnp.arange(cells_all // block_size, dtype=jnp.int32))[0]
    amplitude = amplitude.reshape(ORIENTS, 2, 3, 2, DIRS)
    summed = mueller_sum(amplitude, orient_table, polar_angle, azimuth)
    weight_total = jnp.sum(orient_weights(orient_table)[1])
    return summed / (weight_total * float(GZ * GXY))
```

```python
import functools
import math

import jax
import jax.numpy as jnp
from jax import lax
from jax.experimental import pallas as pl
from jax.experimental.pallas import tpu as pltpu
from jax.sharding import PartitionSpec as P

GX = 96
ORIENT_GRID = 16
THETA_GRID = 180
YL = 8
wave_step = 0.4
MESH = pl.DeviceIdType.MESH
F32 = jnp.float32
BF16 = jnp.bfloat16


def sincos(angle):
    quarter = jnp.round(angle * (2.0 / math.pi))
    rest = angle - quarter * 1.5703125
    rest = rest - quarter * 4.83826794896619e-4
    square = rest * rest
    sine = rest + rest * square * (
        -1.6666654611e-1 + square * (8.3321608736e-3 + square * -1.9515295891e-4)
    )
    cosine = 1.0 - 0.5 * square + square * square * (
        4.166664568298827e-2
        + square * (-1.388731625493765e-3 + square * 2.443315711809948e-5)
    )
    turns = quarter.astype(jnp.int32)
    odd = (turns & 1) == 1
    sin_sign = jnp.where((turns & 2) == 2, -1.0, 1.0)
    cos_sign = jnp.where(((turns + 1) & 2) == 2, -1.0, 1.0)
    return (
        jnp.where(odd, cosine, sine) * sin_sign,
        jnp.where(odd, sine, cosine) * cos_sign,
    )


def flip_index(me, step, size):
    if size & (size - 1):
        return (me + step) % size
    result, bit = 0, 1
    while bit < size:
        result = result + ((me // bit) % 2 + (step // bit) % 2) % 2 * bit
        bit *= 2
    return result


def kernel(
    slab_size, orient_size, planes, cells_all,
    mask_ref, dirs_ref, table_ref, out_ref,
    normal, trig, polar, sent, landed, parts,
    send_sem, recv_sem, part_send, part_recv,
):
    slab = lax.axis_index("slab")
    orient = lax.axis_index("orient")
    rows = mask_ref.shape[1]
    depth = mask_ref.shape[2]
    width = dirs_ref.shape[2]
    group = sent.shape[1] // 2
    pairs = rows // (2 * group)

    barrier = pltpu.get_barrier_semaphore()
    for step in range(1, slab_size):
        pl.semaphore_signal(
            barrier, inc=1, device_id=(orient, flip_index(slab, step, slab_size)),
            device_id_type=MESH,
        )
    for step in range(1, orient_size):
        pl.semaphore_signal(
            barrier, inc=1, device_id=((orient + step) % orient_size, slab),
            device_id_type=MESH,
        )

    dirs = dirs_ref[...].astype(F32)
    sin_p, cos_p = sincos((dirs[:, 0, :] + 0.5) * (math.pi / THETA_GRID))
    sin_a, cos_a = sincos(dirs[:, 1, :] * (2.0 * math.pi / THETA_GRID))
    normal[0] = sin_p * cos_a
    normal[1] = sin_p * sin_a
    normal[2] = cos_p
    polar[0] = sin_p
    polar[1] = cos_p
    polar[2] = sin_a
    polar[3] = cos_a

    line = lax.broadcasted_iota(jnp.int32, (24, 1), 0)
    within = (line % 8).astype(F32)
    coef_x = jnp.where(line < 8, within, jnp.where(line == 16, 8.0, 0.0)) * wave_step
    coef_y = jnp.where(
        (line >= 8) & (line < 16), within,
        jnp.where(line == 17, 2.0 * YL, jnp.where(line == 19, 1.0 * YL, 0.0)),
    ) * wave_step

    def make_tables(index, carry):
        row = pl.ds(index, 1)
        for plane in range(planes):
            depth_at = (slab * planes + plane).astype(F32)
            coef_z = jnp.where((line == 18) | (line == 19), depth_at, 0.0) * wave_step
            angle = (
                coef_x * normal[0, row, :] + coef_y * normal[1, row, :]
                + coef_z * normal[2, row, :]
            )
            sine, cosine = sincos(angle)
            trig[0, plane, index] = cosine
            trig[1, plane, index] = sine
        return carry

    lax.fori_loop(0, slab_size, make_tables, 0)

    def split(values):
        high = values.astype(BF16)
        return high, (values - high.astype(F32)).astype(BF16)

    def chunk(index):
        total = None
        for plane in range(planes):
            cos_t = trig[0, plane, index]
            sin_t = trig[1, plane, index]
            step_c, step_s = cos_t[16:17], sin_t[16:17]
            tile_c, tile_s = cos_t[0:8], sin_t[0:8]
            list_c, list_s = [], []
            for turn in range(GX // 8):
                list_c.append(tile_c)
                list_s.append(tile_s)
                if turn + 1 < GX // 8:
                    tile_c, tile_s = (
                        tile_c * step_c - tile_s * step_s,
                        tile_s * step_c + tile_c * step_s,
                    )
            line_c = jnp.concatenate(list_c, axis=0)
            line_s = jnp.concatenate(list_s, axis=0)
            blocks = [[], [], [], []]
            for y in range(depth // GX):
                y_c, y_s = cos_t[8 + y : 9 + y], sin_t[8 + y : 9 + y]
                c_high, c_low = split(line_c * y_c - line_s * y_s)
                s_high, s_low = split(line_s * y_c + line_c * y_s)
                for held, piece in zip(blocks, (c_high, c_low, s_high, s_low)):
                    held.append(piece)
            c_high, c_low, s_high, s_low = (jnp.concatenate(b, axis=0) for b in blocks)
            masked = mask_ref[plane]
            real = jnp.dot(masked, c_high, preferred_element_type=F32) + jnp.dot(
                masked, c_low, preferred_element_type=F32
            )
            imag = jnp.dot(masked, s_high, preferred_element_type=F32) + jnp.dot(
                masked, s_low, preferred_element_type=F32
            )
            span = 2 * group
            jump_c, jump_s = cos_t[17:18], sin_t[17:18]
            acc_c, acc_s = real[(pairs - 1) * span :], imag[(pairs - 1) * span :]
            for pair in range(pairs - 2, -1, -1):
                part = slice(pair * span, (pair + 1) * span)
                acc_c, acc_s = (
                    acc_c * jump_c - acc_s * jump_s + real[part],
                    acc_s * jump_c + acc_c * jump_s + imag[part],
                )
            lower = lax.broadcasted_iota(jnp.int32, (span, width), 0) < group
            last_c = jnp.where(lower, cos_t[18:19], cos_t[19:20])
            last_s = jnp.where(lower, sin_t[18:19], sin_t[19:20])
            whole_c = acc_c * last_c - acc_s * last_s
            whole_s = acc_s * last_c + acc_c * last_s
            whole_c = whole_c + jnp.concatenate([whole_c[group:], whole_c[:group]], axis=0)
            whole_s = whole_s + jnp.concatenate([whole_s[group:], whole_s[:group]], axis=0)
            here = jnp.where(lower, whole_c, whole_s)
            total = here if total is None else total + here
        return total

    def slab_copy(step):
        peer = flip_index(slab, step, slab_size)
        return pltpu.make_async_remote_copy(
            src_ref=sent.at[step],
            dst_ref=landed.at[step],
            send_sem=send_sem.at[step],
            recv_sem=recv_sem.at[step],
            device_id=(orient, peer),
            device_id_type=MESH,
        )

    pl.semaphore_wait(barrier, slab_size - 1 + orient_size - 1)

    def advance(count, carry):
        step = slab_size - 1 - count
        sent[step] = chunk(flip_index(slab, step, slab_size))
        slab_copy(step).start()
        return carry

    lax.fori_loop(0, slab_size - 1, advance, 0)
    amplitude = chunk(slab)
    for step in range(slab_size - 1, 0, -1):
        slab_copy(step).wait_recv()
        amplitude = amplitude + landed[step]

    weights = sincos((table_ref[...][:, 1:2].astype(F32) + 0.5) * (math.pi / ORIENT_GRID))[0]
    weight_total = jnp.sum(weights, axis=0, keepdims=True)
    local_orients = group // 6
    own = pl.ds(slab, 1)
    sin_p, cos_p = polar[0, own, :], polar[1, own, :]
    sin_a, cos_a = polar[2, own, :], polar[3, own, :]
    own_table = table_ref[pl.ds(orient * local_orients, local_orients), :].astype(F32)
    turn_s, turn_c = sincos(own_table[:, 0:1] * (2.0 * math.pi / ORIENT_GRID))
    own_weight = sincos((own_table[:, 1:2] + 0.5) * (math.pi / ORIENT_GRID))[0]
    results = [0.0, 0.0, 0.0, 0.0]
    for o in range(local_orients):
        t_c, t_s = turn_c[o : o + 1], turn_s[o : o + 1]
        weight = own_weight[o : o + 1]
        cos_q = cos_a * t_c + sin_a * t_s
        sin_q = sin_a * t_c - cos_a * t_s

        def entry(p, c, r):
            at = r * group + o * 6 + p * 3 + c
            return amplitude[at : at + 1]

        def project(p, r):
            first, second, third = entry(p, 0, r), entry(p, 1, r), entry(p, 2, r)
            par = cos_p * (first * cos_q + second * sin_q) - sin_p * third
            across = second * cos_q - first * sin_q
            return par, across

        ul_r, ur_r = project(0, 0)
        ul_i, ur_i = project(0, 1)
        ll_r, lr_r = project(1, 0)
        ll_i, lr_i = project(1, 1)
        lr2 = lr_r * lr_r + lr_i * lr_i
        ul2 = ul_r * ul_r + ul_i * ul_i
        ur2 = ur_r * ur_r + ur_i * ur_i
        ll2 = ll_r * ll_r + ll_i * ll_i
        found = (
            0.5 * (lr2 + ul2 + ur2 + ll2),
            0.5 * (ul2 - lr2 + ll2 - ur2),
            lr_r * ul_r + lr_i * ul_i + ur_r * ll_r + ur_i * ll_i,
            ul_r * lr_i - ul_i * lr_r + ll_r * ur_i - ll_i * ur_r,
        )
        results = [old + weight * new for old, new in zip(results, found)]

    parts[orient] = jnp.concatenate(results, axis=0)

    def part_copy(step):
        return pltpu.make_async_remote_copy(
            src_ref=parts.at[orient],
            dst_ref=parts.at[orient],
            send_sem=part_send.at[step],
            recv_sem=part_recv.at[step],
            device_id=((orient + step) % orient_size, slab),
            device_id_type=MESH,
        )

    for step in range(1, orient_size):
        part_copy(step).start()
    for step in range(slab_size - 1, 0, -1):
        slab_copy(step).wait_send()
    for step in range(1, orient_size):
        back = (orient + orient_size - step) % orient_size
        pltpu.make_async_remote_copy(
            src_ref=parts.at[orient],
            dst_ref=parts.at[back],
            send_sem=part_send.at[step],
            recv_sem=part_recv.at[step],
            device_id=(back, slab),
            device_id_type=MESH,
        ).wait_recv()
    summed = parts[0]
    for o in range(1, orient_size):
        summed = summed + parts[o]
    out_ref[...] = summed / (weight_total * cells_all)
    for step in range(1, orient_size):
        part_copy(step).wait_send()


def shards(slab_size, orient_size, polarization, occupied, orient_table, dir_index):
    orients, _, _, planes, cells = polarization.shape
    group = orients * 6
    depth = YL * GX
    masked = polarization * occupied.astype(BF16)[None, None, None]
    masked = masked.reshape(group, planes, cells // depth, depth)
    masked = masked.transpose(1, 2, 0, 3).reshape(planes, cells // depth * group, depth)
    width = dir_index.shape[0] // slab_size
    dirs = dir_index.T.reshape(2, slab_size, width).transpose(1, 0, 2)
    vmem = pl.BlockSpec(memory_space=pltpu.VMEM)
    return pl.pallas_call(
        functools.partial(
            kernel, slab_size, orient_size, planes, float(planes * slab_size * cells)
        ),
        out_shape=jax.ShapeDtypeStruct((4, width), F32),
        in_specs=[vmem] * 3,
        out_specs=vmem,
        scratch_shapes=[
            pltpu.VMEM((3, slab_size, width), F32),
            pltpu.VMEM((2, planes, slab_size, 24, width), F32),
            pltpu.VMEM((4, slab_size, width), F32),
            pltpu.VMEM((slab_size, 2 * group, width), F32),
            pltpu.VMEM((slab_size, 2 * group, width), F32),
            pltpu.VMEM((orient_size, 4, width), F32),
            pltpu.SemaphoreType.DMA((slab_size,)),
            pltpu.SemaphoreType.DMA((slab_size,)),
            pltpu.SemaphoreType.DMA((orient_size,)),
            pltpu.SemaphoreType.DMA((orient_size,)),
        ],
        compiler_params=pltpu.CompilerParams(collective_id=0, has_side_effects=True),
    )(masked, dirs, orient_table)


def solution(mesh):
    return jax.shard_map(
        functools.partial(shards, mesh.shape["slab"], mesh.shape["orient"]),
        mesh=mesh,
        in_specs=(P("orient", None, None, "slab", None), P("slab", None), P(), P()),
        out_specs=P(None, "slab"),
        check_vma=False,
    )
```

```python
import functools
import math

import jax
import jax.numpy as jnp
from jax import lax
from jax.experimental import pallas as pl
from jax.experimental.pallas import tpu as pltpu
from jax.sharding import PartitionSpec as P

GX = 96
ORIENT_GRID = 16
THETA_GRID = 180
YL = 4
MB = 4
wave_step = 0.4
MESH = pl.DeviceIdType.MESH
F32 = jnp.float32
BF16 = jnp.bfloat16


def sincos(angle):
    quarter = jnp.round(angle * (2.0 / math.pi))
    rest = angle - quarter * 1.5703125
    rest = rest - quarter * 4.83826794896619e-4
    square = rest * rest
    sine = rest + rest * square * (
        -1.6666654611e-1 + square * (8.3321608736e-3 + square * -1.9515295891e-4)
    )
    cosine = 1.0 - 0.5 * square + square * square * (
        4.166664568298827e-2
        + square * (-1.388731625493765e-3 + square * 2.443315711809948e-5)
    )
    turns = quarter.astype(jnp.int32)
    odd = (turns & 1) == 1
    sin_sign = jnp.where((turns & 2) == 2, -1.0, 1.0)
    cos_sign = jnp.where(((turns + 1) & 2) == 2, -1.0, 1.0)
    return (
        jnp.where(odd, cosine, sine) * sin_sign,
        jnp.where(odd, sine, cosine) * cos_sign,
    )


def flip_index(me, step, size):
    if size & (size - 1):
        return (me + step) % size
    result, bit = 0, 1
    while bit < size:
        result = result + ((me // bit) % 2 + (step // bit) % 2) % 2 * bit
        bit *= 2
    return result


def kernel(
    slab_size, orient_size, cells_all,
    table_ref, dirs_ref, pol_ref, occ_ref, out_ref,
    normal, trig, basis, held_pol, held_occ, mask, phases, sent, landed, parts,
    load_sem, send_sem, recv_sem, part_send, part_recv,
):
    slab = lax.axis_index("slab")
    orient = lax.axis_index("orient")
    loads = [
        pltpu.make_async_copy(pol_ref, held_pol, load_sem.at[0]),
        pltpu.make_async_copy(occ_ref, held_occ, load_sem.at[1]),
    ]
    for load in loads:
        load.start()
    local_orients, components, planes, _, cells = pol_ref.shape
    all_orients = table_ref.shape[1]
    width = dirs_ref.shape[2]
    group = sent.shape[1] // 2
    span = 2 * group
    depth = YL * GX
    pairs = cells // depth // 2

    barrier = pltpu.get_barrier_semaphore()
    for step in range(1, slab_size):
        pl.semaphore_signal(
            barrier, inc=1, device_id=(orient, flip_index(slab, step, slab_size)),
            device_id_type=MESH,
        )
    for step in range(1, orient_size):
        pl.semaphore_signal(
            barrier, inc=1, device_id=((orient + step) % orient_size, slab),
            device_id_type=MESH,
        )

    dirs = dirs_ref[...].astype(F32)
    azimuth = dirs[:, 1, :] * (2.0 * math.pi / THETA_GRID)
    sin_p, cos_p = sincos((dirs[:, 0, :] + 0.5) * (math.pi / THETA_GRID))
    sin_a, cos_a = sincos(azimuth)
    normal[0] = sin_p * cos_a
    normal[1] = sin_p * sin_a
    normal[2] = cos_p
    normal[3] = sin_p
    normal[4] = azimuth

    line = lax.broadcasted_iota(jnp.int32, (24, 1), 0)
    middle = 0.5 * (YL - 1)
    coef_x = jnp.where(
        line < 8, line.astype(F32), jnp.where(line == 16, 8.0, 0.0)
    ) * wave_step
    coef_y = jnp.where(
        (line >= 8) & (line < 16), line.astype(F32) - 7.5,
        jnp.where(
            line == 17, 2.0 * YL,
            jnp.where(line == 18, middle, jnp.where(line == 19, YL + middle, 0.0)),
        ),
    ) * wave_step

    together = math.gcd(slab_size, 4)

    def make_tables(block, carry):
        for inner in range(together):
            index = block * together + inner
            row = pl.ds(index, 1)
            for plane in range(planes):
                depth_at = (slab * planes + plane).astype(F32)
                coef_z = jnp.where((line == 18) | (line == 19), depth_at, 0.0) * wave_step
                angle = (
                    coef_x * normal[0, row, :] + coef_y * normal[1, row, :]
                    + coef_z * normal[2, row, :]
                )
                sine, cosine = sincos(angle)
                trig[0, plane, index] = cosine
                trig[1, plane, index] = sine
        return carry

    lax.fori_loop(0, slab_size // together, make_tables, 0)

    tilt_row = lax.broadcasted_iota(jnp.int32, (all_orients, width), 0)
    tilts = jnp.zeros((all_orients, width), F32)
    for o in range(all_orients):
        tilts = jnp.where(tilt_row == o, table_ref[1, o].astype(F32), tilts)
    weights = sincos((tilts + 0.5) * (math.pi / ORIENT_GRID))[0]
    share = 1.0 / (jnp.sum(weights, axis=0, keepdims=True) * cells_all)
    own = pl.ds(slab, 1)
    for o in range(local_orients):
        turn = table_ref[0, orient * local_orients + o].astype(F32)
        tilt = table_ref[1, orient * local_orients + o].astype(F32)
        turns = jnp.full((1, width), turn, F32) * (2.0 * math.pi / ORIENT_GRID)
        sin_q, cos_q = sincos(normal[4, own, :] - turns)
        scaled = (jnp.full((1, width), tilt, F32) + 0.5) * (math.pi / ORIENT_GRID)
        basis[o, 0:1] = sin_q
        basis[o, 1:2] = cos_q
        basis[o, 2:3] = sincos(scaled)[0] * share

    for load in loads:
        load.wait()

    def place(block, carry):
        for plane in range(planes):
            for part in range(MB):
                at = pl.ds(pl.multiple_of((block * MB + part) * depth, 128), depth)
                kept = held_occ[pl.ds(plane, 1), at].astype(F32).astype(BF16)
                for o in range(local_orients):
                    for c in range(components):
                        piece = held_pol[o, c, plane, :, at] * kept
                        first = part * group + (o * components + c) * 2
                        mask[plane, block, first : first + 2, 0:depth] = piece
                        mask[plane, block, first : first + 2, depth : 2 * depth] = piece
        return carry

    lax.fori_loop(0, cells // depth // MB, place, 0)

    def generate(index, plane, slot):
        cos_t = trig[0, plane, index]
        sin_t = trig[1, plane, index]
        step_c, step_s = cos_t[16:17], sin_t[16:17]
        tile_c, tile_s = cos_t[0:8], sin_t[0:8]

        def put(kind, first, values):
            high = values.astype(BF16)
            phases[slot, kind, first : first + 16] = high
            phases[slot, kind, depth + first : depth + first + 16] = (
                values - high.astype(F32)
            ).astype(BF16)

        for turn in range(GX // 16):
            next_c = tile_c * step_c - tile_s * step_s
            next_s = tile_s * step_c + tile_c * step_s
            line_c = jnp.concatenate([tile_c, next_c], axis=0)
            line_s = jnp.concatenate([tile_s, next_s], axis=0)
            for y in range(YL // 2):
                y_c, y_s = cos_t[8 + y : 9 + y], sin_t[8 + y : 9 + y]
                cc, ss = line_c * y_c, line_s * y_s
                sc, cs = line_s * y_c, line_c * y_s
                above = (YL // 2 + y) * GX + turn * 16
                below = (YL // 2 - 1 - y) * GX + turn * 16
                put(0, above, cc - ss)
                put(0, below, cc + ss)
                put(1, above, sc + cs)
                put(1, below, sc - cs)
            if turn + 1 < GX // 16:
                tile_c = next_c * step_c - next_s * step_s
                tile_s = next_s * step_c + next_c * step_s

    def multiply(index, plane, slot):
        masked = mask[plane].reshape(pairs * span, 2 * depth)
        real = jnp.dot(masked, phases[slot, 0], preferred_element_type=F32)
        imag = jnp.dot(masked, phases[slot, 1], preferred_element_type=F32)
        cos_t = trig[0, plane, index]
        sin_t = trig[1, plane, index]
        jump_c, jump_s = cos_t[17:18], sin_t[17:18]
        acc_c, acc_s = real[(pairs - 1) * span :], imag[(pairs - 1) * span :]
        for pair in range(pairs - 2, -1, -1):
            part = slice(pair * span, (pair + 1) * span)
            acc_c, acc_s = (
                acc_c * jump_c - acc_s * jump_s + real[part],
                acc_s * jump_c + acc_c * jump_s + imag[part],
            )
        lower = lax.broadcasted_iota(jnp.int32, (span, width), 0) < group
        last_c = jnp.where(lower, cos_t[18:19], cos_t[19:20])
        last_s = jnp.where(lower, sin_t[18:19], sin_t[19:20])
        whole_c = acc_c * last_c - acc_s * last_s
        whole_s = acc_s * last_c + acc_c * last_s
        whole_c = whole_c + jnp.concatenate([whole_c[group:], whole_c[:group]], axis=0)
        whole_s = whole_s + jnp.concatenate([whole_s[group:], whole_s[:group]], axis=0)
        return jnp.where(lower, whole_c, whole_s)

    def slab_copy(step):
        peer = flip_index(slab, step, slab_size)
        return pltpu.make_async_remote_copy(
            src_ref=sent.at[step],
            dst_ref=landed.at[step],
            send_sem=send_sem.at[step],
            recv_sem=recv_sem.at[step],
            device_id=(orient, peer),
            device_id_type=MESH,
        )

    def target(count):
        return flip_index(slab, slab_size - 1 - count, slab_size)

    def stage(count, slot, last):
        index = target(count)
        step = slab_size - 1 - count
        total = None
        for plane in range(planes):
            now = (slot + plane) % 2
            if plane + 1 < planes:
                generate(index, plane + 1, 1 - now)
            elif not last:
                generate(target(count + 1), 0, 1 - now)
            here = multiply(index, plane, now)
            total = here if total is None else total + here
        sent[step] = total
        if not last:
            slab_copy(step).start()

    def advance(turn, carry):
        stage(2 * turn, 0, False)
        stage(2 * turn + 1, planes % 2, False)
        return carry

    generate(target(0), 0, 0)
    pl.semaphore_wait(barrier, slab_size - 1 + orient_size - 1)
    lax.fori_loop(0, slab_size // 2 - 1, advance, 0)
    stage(slab_size - 2, 0, False)
    stage(slab_size - 1, planes % 2, True)

    amplitude = sent[0]
    for step in range(slab_size - 1, 0, -1):
        slab_copy(step).wait_recv()
        amplitude = amplitude + landed[step]

    sin_p, cos_p = normal[3, own, :], normal[2, own, :]
    results = [0.0, 0.0, 0.0, 0.0]
    for o in range(local_orients):
        sin_q, cos_q, weight = basis[o, 0:1], basis[o, 1:2], basis[o, 2:3]

        def entry(p, c, r):
            at = r * group + (o * 3 + c) * 2 + p
            return amplitude[at : at + 1]

        def project(p, r):
            first, second, third = entry(p, 0, r), entry(p, 1, r), entry(p, 2, r)
            par = cos_p * (first * cos_q + second * sin_q) - sin_p * third
            across = second * cos_q - first * sin_q
            return par, across

        ul_r, ur_r = project(0, 0)
        ul_i, ur_i = project(0, 1)
        ll_r, lr_r = project(1, 0)
        ll_i, lr_i = project(1, 1)
        lr2 = lr_r * lr_r + lr_i * lr_i
        ul2 = ul_r * ul_r + ul_i * ul_i
        ur2 = ur_r * ur_r + ur_i * ur_i
        ll2 = ll_r * ll_r + ll_i * ll_i
        found = (
            0.5 * (lr2 + ul2 + ur2 + ll2),
            0.5 * (ul2 - lr2 + ll2 - ur2),
            lr_r * ul_r + lr_i * ul_i + ur_r * ll_r + ur_i * ll_i,
            ul_r * lr_i - ul_i * lr_r + ll_r * ur_i - ll_i * ur_r,
        )
        results = [old + weight * new for old, new in zip(results, found)]

    parts[orient] = jnp.concatenate(results, axis=0)

    def part_copy(step):
        return pltpu.make_async_remote_copy(
            src_ref=parts.at[orient],
            dst_ref=parts.at[orient],
            send_sem=part_send.at[step],
            recv_sem=part_recv.at[step],
            device_id=((orient + step) % orient_size, slab),
            device_id_type=MESH,
        )

    for step in range(1, orient_size):
        part_copy(step).start()
    for step in range(slab_size - 1, 0, -1):
        slab_copy(step).wait_send()
    for step in range(1, orient_size):
        back = (orient + orient_size - step) % orient_size
        pltpu.make_async_remote_copy(
            src_ref=parts.at[orient],
            dst_ref=parts.at[back],
            send_sem=part_send.at[step],
            recv_sem=part_recv.at[step],
            device_id=(back, slab),
            device_id_type=MESH,
        ).wait_recv()
    summed = parts[0]
    for o in range(1, orient_size):
        summed = summed + parts[o]
    out_ref[...] = summed
    for step in range(1, orient_size):
        part_copy(step).wait_send()


def shards(slab_size, orient_size, polarization, occupied, orient_table, dir_index):
    orients, _, components, planes, cells = polarization.shape
    group = orients * 6
    depth = YL * GX
    pol = polarization.transpose(0, 2, 3, 1, 4)
    width = dir_index.shape[0] // slab_size
    dirs = dir_index.T.reshape(2, slab_size, width).transpose(1, 0, 2)
    vmem = pl.BlockSpec(memory_space=pltpu.VMEM)
    anywhere = pl.BlockSpec(memory_space=pltpu.HBM)
    return pl.pallas_call(
        functools.partial(
            kernel, slab_size, orient_size, float(planes * slab_size * cells)
        ),
        out_shape=jax.ShapeDtypeStruct((4, width), F32),
        in_specs=[pl.BlockSpec(memory_space=pltpu.SMEM), vmem, anywhere, anywhere],
        out_specs=vmem,
        scratch_shapes=[
            pltpu.VMEM((5, slab_size, width), F32),
            pltpu.VMEM((2, planes, slab_size, 24, width), F32),
            pltpu.VMEM((orients, 3, width), F32),
            pltpu.VMEM(pol.shape, BF16),
            pltpu.VMEM(occupied.shape, jnp.int32),
            pltpu.VMEM((planes, cells // depth // MB, MB * group, 2 * depth), BF16),
            pltpu.VMEM((2, 2, 2 * depth, width), BF16),
            pltpu.VMEM((slab_size, 2 * group, width), F32),
            pltpu.VMEM((slab_size, 2 * group, width), F32),
            pltpu.VMEM((orient_size, 4, width), F32),
            pltpu.SemaphoreType.DMA((2,)),
            pltpu.SemaphoreType.DMA((slab_size,)),
            pltpu.SemaphoreType.DMA((slab_size,)),
            pltpu.SemaphoreType.DMA((orient_size,)),
            pltpu.SemaphoreType.DMA((orient_size,)),
        ],
        compiler_params=pltpu.CompilerParams(
            collective_id=0, has_side_effects=True
        ),
    )(orient_table.T, dirs, pol, occupied)


def solution(mesh):
    return jax.shard_map(
        functools.partial(shards, mesh.shape["slab"], mesh.shape["orient"]),
        mesh=mesh,
        in_specs=(P("orient", None, None, "slab", None), P("slab", None), P(), P()),
        out_specs=P(None, "slab"),
        check_vma=False,
    )
```

```python
import functools
import math

import jax
import jax.numpy as jnp
from jax import lax
from jax.experimental import pallas as pl
from jax.experimental.pallas import tpu as pltpu
from jax.sharding import PartitionSpec as P

GX = 96
ORIENT_GRID = 16
THETA_GRID = 180
YL = 4
MB = 4
wave_step = 0.4
MESH = pl.DeviceIdType.MESH
F32 = jnp.float32
BF16 = jnp.bfloat16


def sincos(angle):
    quarter = jnp.round(angle * (2.0 / math.pi))
    rest = angle - quarter * 1.5703125
    rest = rest - quarter * 4.83826794896619e-4
    square = rest * rest
    sine = rest + rest * square * (
        -1.6666654611e-1 + square * (8.3321608736e-3 + square * -1.9515295891e-4)
    )
    cosine = 1.0 - 0.5 * square + square * square * (
        4.166664568298827e-2
        + square * (-1.388731625493765e-3 + square * 2.443315711809948e-5)
    )
    turns = quarter.astype(jnp.int32)
    odd = (turns & 1) == 1
    sin_sign = jnp.where((turns & 2) == 2, -1.0, 1.0)
    cos_sign = jnp.where(((turns + 1) & 2) == 2, -1.0, 1.0)
    return (
        jnp.where(odd, cosine, sine) * sin_sign,
        jnp.where(odd, sine, cosine) * cos_sign,
    )


def flip_index(me, step, size):
    if size & (size - 1):
        return (me + step) % size
    result, bit = 0, 1
    while bit < size:
        result = result + ((me // bit) % 2 + (step // bit) % 2) % 2 * bit
        bit *= 2
    return result


def kernel(
    slab_size, orient_size, cells_all,
    table_hbm, dirs_hbm, pol_ref, occ_ref, out_ref,
    table_ref, dirs_ref, normal, trig, basis, held_pol, held_occ, mask, phases, sent, landed, parts,
    load_sem, send_sem, recv_sem, part_send, part_recv,
):
    slab = lax.axis_index("slab")
    orient = lax.axis_index("orient")
    loads = [
        pltpu.make_async_copy(dirs_hbm, dirs_ref, load_sem.at[2]),
        pltpu.make_async_copy(table_hbm, table_ref, load_sem.at[3]),
        pltpu.make_async_copy(pol_ref, held_pol, load_sem.at[0]),
        pltpu.make_async_copy(occ_ref, held_occ, load_sem.at[1]),
    ]
    for load in loads:
        load.start()
    local_orients, components, planes, _, cells = pol_ref.shape
    all_orients = table_ref.shape[1]
    width = dirs_ref.shape[2]
    group = sent.shape[1] // 2
    span = 2 * group
    depth = YL * GX
    pairs = cells // depth // 2

    barrier = pltpu.get_barrier_semaphore()
    for step in range(1, slab_size):
        pl.semaphore_signal(
            barrier, inc=1, device_id=(orient, flip_index(slab, step, slab_size)),
            device_id_type=MESH,
        )
    for step in range(1, orient_size):
        pl.semaphore_signal(
            barrier, inc=1, device_id=((orient + step) % orient_size, slab),
            device_id_type=MESH,
        )

    loads[0].wait()
    dirs = dirs_ref[...].astype(F32)
    azimuth = dirs[:, 1, :] * (2.0 * math.pi / THETA_GRID)
    sin_p, cos_p = sincos((dirs[:, 0, :] + 0.5) * (math.pi / THETA_GRID))
    sin_a, cos_a = sincos(azimuth)
    normal[0] = sin_p * cos_a
    normal[1] = sin_p * sin_a
    normal[2] = cos_p
    normal[3] = sin_p
    normal[4] = azimuth

    line = lax.broadcasted_iota(jnp.int32, (24, 1), 0)
    middle = 0.5 * (YL - 1)
    coef_x = jnp.where(
        line < 8, line.astype(F32), jnp.where(line == 16, 8.0, 0.0)
    ) * wave_step
    coef_y = jnp.where(
        (line >= 8) & (line < 16), line.astype(F32) - 7.5,
        jnp.where(
            line == 17, 2.0 * YL,
            jnp.where(line == 18, middle, jnp.where(line == 19, YL + middle, 0.0)),
        ),
    ) * wave_step

    together = math.gcd(slab_size, 4)

    def make_tables(block, carry):
        for inner in range(together):
            index = block * together + inner
            row = pl.ds(index, 1)
            for plane in range(planes):
                depth_at = (slab * planes + plane).astype(F32)
                coef_z = jnp.where((line == 18) | (line == 19), depth_at, 0.0) * wave_step
                angle = (
                    coef_x * normal[0, row, :] + coef_y * normal[1, row, :]
                    + coef_z * normal[2, row, :]
                )
                sine, cosine = sincos(angle)
                trig[0, plane, index] = cosine
                trig[1, plane, index] = sine
        return carry

    lax.fori_loop(0, slab_size // together, make_tables, 0)

    loads[1].wait()
    tilt_row = lax.broadcasted_iota(jnp.int32, (all_orients, width), 0)
    tilts = jnp.zeros((all_orients, width), F32)
    for o in range(all_orients):
        tilts = jnp.where(tilt_row == o, table_ref[1, o].astype(F32), tilts)
    weights = sincos((tilts + 0.5) * (math.pi / ORIENT_GRID))[0]
    share = 1.0 / (jnp.sum(weights, axis=0, keepdims=True) * cells_all)
    own = pl.ds(slab, 1)
    for o in range(local_orients):
        turn = table_ref[0, orient * local_orients + o].astype(F32)
        tilt = table_ref[1, orient * local_orients + o].astype(F32)
        turns = jnp.full((1, width), turn, F32) * (2.0 * math.pi / ORIENT_GRID)
        sin_q, cos_q = sincos(normal[4, own, :] - turns)
        scaled = (jnp.full((1, width), tilt, F32) + 0.5) * (math.pi / ORIENT_GRID)
        basis[o, 0:1] = sin_q
        basis[o, 1:2] = cos_q
        basis[o, 2:3] = sincos(scaled)[0] * share

    for load in loads[2:]:
        load.wait()

    def place(block, carry):
        for plane in range(planes):
            for part in range(MB):
                at = pl.ds(pl.multiple_of((block * MB + part) * depth, 128), depth)
                kept = held_occ[pl.ds(plane, 1), at].astype(F32).astype(BF16)
                pieces = [
                    held_pol[o, c, plane, :, at]
                    for o in range(local_orients)
                    for c in range(components)
                ]
                rows = jnp.concatenate(pieces, axis=0) * kept
                mask[plane, block, part * group : (part + 1) * group, :] = rows
        return carry

    lax.fori_loop(0, cells // depth // MB, place, 0)

    def generate(index, plane, slot):
        cos_t = trig[0, plane, index]
        sin_t = trig[1, plane, index]
        step_c, step_s = cos_t[16:17], sin_t[16:17]
        tile_c, tile_s = cos_t[0:8], sin_t[0:8]

        def put(kind, first, values):
            high = values.astype(BF16)
            phases[slot, kind, first : first + 16] = high
            phases[slot, kind, depth + first : depth + first + 16] = (
                values - high.astype(F32)
            ).astype(BF16)

        for turn in range(GX // 16):
            next_c = tile_c * step_c - tile_s * step_s
            next_s = tile_s * step_c + tile_c * step_s
            line_c = jnp.concatenate([tile_c, next_c], axis=0)
            line_s = jnp.concatenate([tile_s, next_s], axis=0)
            for y in range(YL // 2):
                y_c, y_s = cos_t[8 + y : 9 + y], sin_t[8 + y : 9 + y]
                cc, ss = line_c * y_c, line_s * y_s
                sc, cs = line_s * y_c, line_c * y_s
                above = (YL // 2 + y) * GX + turn * 16
                below = (YL // 2 - 1 - y) * GX + turn * 16
                put(0, above, cc - ss)
                put(0, below, cc + ss)
                put(1, above, sc + cs)
                put(1, below, sc - cs)
            if turn + 1 < GX // 16:
                tile_c = next_c * step_c - next_s * step_s
                tile_s = next_s * step_c + next_c * step_s

    def multiply(index, plane, slot):
        masked = mask[plane].reshape(pairs * span, depth)
        masked = jnp.concatenate([masked, masked], axis=1)
        real = jnp.dot(masked, phases[slot, 0], preferred_element_type=F32)
        imag = jnp.dot(masked, phases[slot, 1], preferred_element_type=F32)
        cos_t = trig[0, plane, index]
        sin_t = trig[1, plane, index]
        jump_c, jump_s = cos_t[17:18], sin_t[17:18]
        acc_c, acc_s = real[(pairs - 1) * span :], imag[(pairs - 1) * span :]
        for pair in range(pairs - 2, -1, -1):
            part = slice(pair * span, (pair + 1) * span)
            acc_c, acc_s = (
                acc_c * jump_c - acc_s * jump_s + real[part],
                acc_s * jump_c + acc_c * jump_s + imag[part],
            )
        lower = lax.broadcasted_iota(jnp.int32, (span, width), 0) < group
        last_c = jnp.where(lower, cos_t[18:19], cos_t[19:20])
        last_s = jnp.where(lower, sin_t[18:19], sin_t[19:20])
        whole_c = acc_c * last_c - acc_s * last_s
        whole_s = acc_s * last_c + acc_c * last_s
        whole_c = whole_c + jnp.concatenate([whole_c[group:], whole_c[:group]], axis=0)
        whole_s = whole_s + jnp.concatenate([whole_s[group:], whole_s[:group]], axis=0)
        return jnp.where(lower, whole_c, whole_s)

    def slab_copy(step):
        peer = flip_index(slab, step, slab_size)
        return pltpu.make_async_remote_copy(
            src_ref=sent.at[step],
            dst_ref=landed.at[step],
            send_sem=send_sem.at[step],
            recv_sem=recv_sem.at[step],
            device_id=(orient, peer),
            device_id_type=MESH,
        )

    def target(count):
        return flip_index(slab, slab_size - 1 - count, slab_size)

    def stage(count, slot, last):
        index = target(count)
        step = slab_size - 1 - count
        total = None
        for plane in range(planes):
            now = (slot + plane) % 2
            if plane + 1 < planes:
                generate(index, plane + 1, 1 - now)
            elif not last:
                generate(target(count + 1), 0, 1 - now)
            here = multiply(index, plane, now)
            total = here if total is None else total + here
        sent[step] = total
        if not last:
            slab_copy(step).start()

    def advance(turn, carry):
        stage(2 * turn, 0, False)
        stage(2 * turn + 1, planes % 2, False)
        return carry

    generate(target(0), 0, 0)
    pl.semaphore_wait(barrier, slab_size - 1 + orient_size - 1)
    lax.fori_loop(0, slab_size // 2 - 1, advance, 0)
    stage(slab_size - 2, 0, False)
    stage(slab_size - 1, planes % 2, True)

    amplitude = sent[0]
    for step in range(slab_size - 1, 0, -1):
        slab_copy(step).wait_recv()
        amplitude = amplitude + landed[step]

    sin_p, cos_p = normal[3, own, :], normal[2, own, :]
    results = [0.0, 0.0, 0.0, 0.0]
    for o in range(local_orients):
        sin_q, cos_q, weight = basis[o, 0:1], basis[o, 1:2], basis[o, 2:3]

        def entry(p, c, r):
            at = r * group + (o * 3 + c) * 2 + p
            return amplitude[at : at + 1]

        def project(p, r):
            first, second, third = entry(p, 0, r), entry(p, 1, r), entry(p, 2, r)
            par = cos_p * (first * cos_q + second * sin_q) - sin_p * third
            across = second * cos_q - first * sin_q
            return par, across

        ul_r, ur_r = project(0, 0)
        ul_i, ur_i = project(0, 1)
        ll_r, lr_r = project(1, 0)
        ll_i, lr_i = project(1, 1)
        lr2 = lr_r * lr_r + lr_i * lr_i
        ul2 = ul_r * ul_r + ul_i * ul_i
        ur2 = ur_r * ur_r + ur_i * ur_i
        ll2 = ll_r * ll_r + ll_i * ll_i
        found = (
            0.5 * (lr2 + ul2 + ur2 + ll2),
            0.5 * (ul2 - lr2 + ll2 - ur2),
            lr_r * ul_r + lr_i * ul_i + ur_r * ll_r + ur_i * ll_i,
            ul_r * lr_i - ul_i * lr_r + ll_r * ur_i - ll_i * ur_r,
        )
        results = [old + weight * new for old, new in zip(results, found)]

    parts[orient] = jnp.concatenate(results, axis=0)

    def part_copy(step):
        return pltpu.make_async_remote_copy(
            src_ref=parts.at[orient],
            dst_ref=parts.at[orient],
            send_sem=part_send.at[step],
            recv_sem=part_recv.at[step],
            device_id=((orient + step) % orient_size, slab),
            device_id_type=MESH,
        )

    for step in range(1, orient_size):
        part_copy(step).start()
    for step in range(slab_size - 1, 0, -1):
        slab_copy(step).wait_send()
    for step in range(1, orient_size):
        back = (orient + orient_size - step) % orient_size
        pltpu.make_async_remote_copy(
            src_ref=parts.at[orient],
            dst_ref=parts.at[back],
            send_sem=part_send.at[step],
            recv_sem=part_recv.at[step],
            device_id=(back, slab),
            device_id_type=MESH,
        ).wait_recv()
    summed = parts[0]
    for o in range(1, orient_size):
        summed = summed + parts[o]
    out_ref[...] = summed
    for step in range(1, orient_size):
        part_copy(step).wait_send()


def shards(slab_size, orient_size, polarization, occupied, orient_table, dir_index):
    orients, _, components, planes, cells = polarization.shape
    group = orients * 6
    depth = YL * GX
    pol = polarization.transpose(0, 2, 3, 1, 4)
    width = dir_index.shape[0] // slab_size
    dirs = dir_index.T.reshape(2, slab_size, width).transpose(1, 0, 2)
    vmem = pl.BlockSpec(memory_space=pltpu.VMEM)
    anywhere = pl.BlockSpec(memory_space=pltpu.HBM)
    return pl.pallas_call(
        functools.partial(
            kernel, slab_size, orient_size, float(planes * slab_size * cells)
        ),
        out_shape=pltpu.VMEM((4, width), F32),
        in_specs=[anywhere] * 4,
        out_specs=vmem,
        scratch_shapes=[
            pltpu.SMEM((2, orient_table.shape[0]), jnp.int32),
            pltpu.VMEM(dirs.shape, jnp.int32),
            pltpu.VMEM((5, slab_size, width), F32),
            pltpu.VMEM((2, planes, slab_size, 24, width), F32),
            pltpu.VMEM((orients, 3, width), F32),
            pltpu.VMEM(pol.shape, BF16),
            pltpu.VMEM(occupied.shape, jnp.int32),
            pltpu.VMEM((planes, cells // depth // MB, MB * group, depth), BF16),
            pltpu.VMEM((2, 2, 2 * depth, width), BF16),
            pltpu.VMEM((slab_size, 2 * group, width), F32),
            pltpu.VMEM((slab_size, 2 * group, width), F32),
            pltpu.VMEM((orient_size, 4, width), F32),
            pltpu.SemaphoreType.DMA((4,)),
            pltpu.SemaphoreType.DMA((slab_size,)),
            pltpu.SemaphoreType.DMA((slab_size,)),
            pltpu.SemaphoreType.DMA((orient_size,)),
            pltpu.SemaphoreType.DMA((orient_size,)),
        ],
        compiler_params=pltpu.CompilerParams(
            collective_id=0, has_side_effects=True
        ),
    )(orient_table.T, dirs, pol, occupied)


def solution(mesh):
    return jax.shard_map(
        functools.partial(shards, mesh.shape["slab"], mesh.shape["orient"]),
        mesh=mesh,
        in_specs=(P("orient", None, None, "slab", None), P("slab", None), P(), P()),
        out_specs=P(None, "slab"),
        check_vma=False,
    )
```
